32 devices in a mesh: blk: 16 (over z, x, core), ang: 2 (over y).
Axes of the slice: x: 2, y: 2, z: 4, core: 2. Of those that a mesh axis runs over, the one named last changes fastest.
Arguments:
- coeffs: bfloat16 [4096, 2048], P('blk'), may hold values from -6 to 6
- orders: int32 [1024], replicated, may hold values from 0 to 47
- plan: int32 [2], replicated, may hold values from 1 to 15
Outputs:
- scores: float32 [2, 4096, 256], P(None, ('blk', 'ang'))
The draws below stay inside these ranges and needn't reach their ends.
Inputs may be any that keep to these rules, and one draw needn't show every extreme that they name: In round r, block b is paired with block b XOR plan[r].
All inputs are finite; a program needn't handle non-finite values.
Results may differ from the reference program's by a relative error of at most 0.002.
Values may be sent and summed in bfloat16 or wider, within the bound.
A program may use at most 64 MiB of HBM per device.

```python
import math
import jax
import jax.numpy as jnp
from jax import lax

IMG_DEV = 256
COEF = 2048
ANGLES = 128
ORDERS = 48
ROUNDS = 2
HALF = 1024
IMAGES = 4096
N_BLK = 16


def with_ends(entries, stream_key, least, high):
    longest = entries.shape.index(max(entries.shape))
    spots = []
    for shift in (0, 1):
        where = [jax.random.randint(jax.random.fold_in(stream_key, axis), (), 0, length) for axis, length in enumerate(entries.shape)]
        where[longest] = (where[longest] + shift) % entries.shape[longest]
        spots.append(tuple(where))
    return entries.at[spots[0]].set(least).at[spots[1]].set(high)


def shard_levels(key, extent, pieces, smallest, largest):
    level, own = 1.0, jax.random.fold_in(key, 6)
    for axis_at, parts in pieces:
        draws = jnp.exp(jax.random.uniform(jax.random.fold_in(own, axis_at), (parts,), jnp.float32, smallest / len(pieces), largest / len(pieces)))
        level = level * jnp.repeat(draws, extent[axis_at] // parts).reshape([-1 if axis == axis_at else 1 for axis in range(len(extent))])
    return level


def normal_values(rng, extent, deviation, reach, pieces=(), kind=jnp.bfloat16):
    loudness = shard_levels(rng, extent, pieces, -0.22, 0.18) if pieces else 1.0
    array = jax.random.normal(rng, extent, jnp.float32) * deviation * loudness
    return jnp.minimum(jnp.maximum(array, -reach), reach).astype(kind)


def setup_inputs(seed: int = 0) -> dict:
    key_of = jax.random.split(jax.random.key(seed), 4)
    return {
        "coeffs": normal_values(key_of[0], (IMAGES, COEF), 1.0, 6.0, ((0, 16),)),
        "orders": with_ends(jax.random.randint(key_of[1], (HALF,), 0, ORDERS), jax.random.fold_in(key_of[1], 1), 0, ORDERS - 1).astype(jnp.int32),
        "plan": jax.random.randint(key_of[2], (ROUNDS,), 1, N_BLK).astype(jnp.int32),
    }


def rotate_rows(block, orders, first_angle, angle_count):
    half_width = block.shape[1] // 2
    real_part = block[:, :half_width].astype(jnp.float32)
    imag_part = block[:, half_width:].astype(jnp.float32)
    angles = (jnp.arange(angle_count) + first_angle).astype(jnp.float32) * (2.0 * math.pi / ANGLES)
    phases = angles[:, None] * orders.astype(jnp.float32)[None, :]
    cosine_table = jnp.cos(phases)[:, None, :]
    sine_table = jnp.sin(phases)[:, None, :]
    rot_real = real_part[None] * cosine_table - imag_part[None] * sine_table
    rot_imag = real_part[None] * sine_table + imag_part[None] * cosine_table
    return jnp.concatenate([rot_real, rot_imag], axis=2).astype(jnp.bfloat16)

def block_best(own_block, partner, orders):
    group_size = 8
    row_count = own_block.shape[0]
    partner_wide = partner.astype(jnp.float32)

    def step(running, step_index):
        rotated = rotate_rows(own_block, orders, step_index * group_size, group_size).astype(jnp.float32)
        stacked = rotated.reshape(group_size * row_count, -1)
        scores_raw = jnp.dot(stacked, partner_wide.T, precision=lax.Precision.HIGHEST, preferred_element_type=jnp.float32)
        return (jnp.maximum(running, scores_raw.reshape(group_size, row_count, -1).max(0)), None)
    start = jnp.full((row_count, partner.shape[0]), -jnp.inf, jnp.float32)
    running, _ = lax.scan(step, start, jnp.arange(ANGLES // group_size, dtype=jnp.int32))
    return running

def reference(coeffs, orders, plan):
    blocks = coeffs.reshape(N_BLK, IMG_DEV, COEF)
    scales = jnp.sqrt(lax.optimization_barrier(jnp.mean(jnp.square(coeffs.astype(jnp.float32)), axis=1)) + 1e-06).reshape(N_BLK, IMG_DEV)
    block_ids = jnp.arange(N_BLK, dtype=jnp.int32)
    round_scores = []
    for round_index in range(ROUNDS):
        partner_ids = jnp.bitwise_xor(block_ids, plan[round_index])

        def per_block(block_index):
            mate = partner_ids[block_index]
            running = block_best(blocks[block_index], blocks[mate], orders)
            return running / (math.sqrt(COEF) * scales[block_index][:, None] * scales[mate][None, :])
        round_scores.append(lax.map(per_block, block_ids).reshape(IMAGES, IMG_DEV))
    return jnp.stack(round_scores)
```

```python
import functools
import math

import jax
import jax.numpy as jnp
import numpy as np
from jax import lax
from jax.experimental import pallas as pl
from jax.experimental.pallas import tpu as pltpu
from jax.sharding import PartitionSpec as P

ANGLES = 128
ORDERS = 48
ROUNDS = 2
LANES = 128
PITCH = 104
MOST_ROUTES = 128
NT = (((1,), (1,)), ((), ()))


def side_mask(p, q):
    for mask in range(1, 1 << max(p, q).bit_length()):
        if bin(mask & p).count("1") % 2 and bin(mask & q).count("1") % 2:
            return mask
    raise ValueError


def routes(n_blk):
    index = np.zeros((n_blk, n_blk), np.int32)
    there, back, sides = [], [], []
    for p in range(1, n_blk):
        for q in range(p, n_blk):
            index[p, q] = index[q, p] = len(there)
            mask = side_mask(p, q)
            side = [bin(mask & b).count("1") % 2 for b in range(n_blk)]
            pairs = [(b, b ^ (q if side[b] else p)) for b in range(n_blk)]
            there.append(pairs)
            back.append([(t, s) for s, t in pairs])
            sides.append(side)
    return index, there, back, np.array(sides, np.int32)


def angle_table():
    theta = 2.0 * math.pi * np.arange(ANGLES) / ANGLES
    phase = theta[:, None] * np.arange(ORDERS)[None, :]
    full = np.concatenate([np.cos(phase), np.sin(phase)], axis=1)
    high = full.astype(np.float32).astype(jnp.bfloat16)
    low = (full - high.astype(np.float64)).astype(np.float32).astype(jnp.bfloat16)
    return np.concatenate([high, low], axis=1)


def sort_kernel(info, orders_ref, x_ref, own_ref, send_ref, perm):
    half = orders_ref.shape[1]
    rows = x_ref.shape[0]
    chunks = half // LANES
    slot = lax.broadcasted_iota(jnp.int32, (1, half), 1)
    key = (orders_ref[...] * half + slot).astype(jnp.float32)
    lane = lax.broadcasted_iota(jnp.int32, (LANES, half), 1).astype(jnp.float32)
    for c in range(chunks):
        piece = key[:, c * LANES : (c + 1) * LANES]
        column = jnp.broadcast_to(piece, (LANES, LANES)).T
        count = jnp.zeros((LANES, LANES), jnp.float32)
        for d in range(chunks):
            other = key[:, d * LANES : (d + 1) * LANES]
            count += jnp.where(other < column, 1.0, 0.0)
        rank = jnp.sum(count, axis=1, keepdims=True)
        perm[c * LANES : (c + 1) * LANES, :] = jnp.where(lane == rank, 1.0, 0.0).astype(jnp.bfloat16)
    width = 2 * LANES
    for d in range(half // width):
        p = perm[:, d * width : (d + 1) * width]
        for part in range(2):
            got = jnp.dot(
                x_ref[:, part * half : (part + 1) * half], p, preferred_element_type=jnp.float32
            ).astype(jnp.bfloat16)
            for e in range(2):
                at = ((2 * d + e) * 2 + part) * LANES
                own_ref[:, at : at + LANES] = got[:, e * LANES : (e + 1) * LANES]
    share = send_ref.shape[0]
    first = pl.multiple_of(info[0] * share, share)
    send_ref[...] = own_ref[pl.ds(first, share), :]


def pair_kernel(info, own_ref, mate_ref, table_ref, mine_ref, other_ref, turned_ref, grid, acc, best):
    rows, cols = own_ref.shape
    mates = mate_ref.shape[0]
    width = 2 * LANES
    slots = lax.broadcasted_iota(jnp.int32, (1, LANES), 1)

    def product(chunk, low, high):
        at = pl.multiple_of(chunk * width, width)
        place = slots + chunk * LANES
        keep = jnp.where((place >= low) & (place < high), 1.0, 0.0).astype(jnp.bfloat16)
        u = mate_ref[:, pl.ds(at, LANES)] * keep
        v = mate_ref[:, pl.ds(at + LANES, LANES)] * keep
        w = jnp.concatenate(
            [jnp.concatenate([u, v], axis=1), jnp.concatenate([v, -u], axis=1)], axis=0
        )
        return lax.dot_general(
            own_ref[:, pl.ds(at, width)], w, NT, preferred_element_type=jnp.float32
        )

    def spread(k, value):
        for i in range(0, rows, 8):
            grid[pl.ds(i * PITCH + k, 8, stride=PITCH), :] = value[i : i + 8, :mates]
            grid[pl.ds(i * PITCH + k + ORDERS, 8, stride=PITCH), :] = value[i : i + 8, mates:]

    def order_step(k, carry):
        low, high = info[1 + k], info[2 + k]
        chunk = jnp.minimum(low // LANES, cols // width - 1)
        last = (high + LANES - 1) // LANES
        value = product(chunk, low, high)
        spread(k, value)

        @pl.when(last > chunk + 1)
        def _():
            acc[...] = value

            def more(c, carry):
                acc[...] += product(c, low, high)
                return carry

            lax.fori_loop(chunk + 1, last, more, 0)
            spread(k, acc[...])

        return carry

    lax.fori_loop(0, ORDERS, order_step, 0)

    table = table_ref[...]

    def image_step(step, carry):
        base = pl.multiple_of(step * 8, 8)
        rows_out = []
        for i in range(0, 8, 2):
            pieces = []
            for e in range(2):
                at = pl.multiple_of((base + i + e) * PITCH, 8)
                pieces.append(grid[pl.ds(at, 2 * ORDERS), :].astype(jnp.bfloat16))
            d = jnp.concatenate(pieces, axis=1)
            d = jnp.concatenate([d, d], axis=0)
            raw = jnp.dot(table, d, preferred_element_type=jnp.float32)
            top = jnp.max(raw, axis=0, keepdims=True)
            rows_out += [top[:, :mates], top[:, mates:]]
        best[pl.ds(base, 8), :] = jnp.concatenate(rows_out, axis=0)
        return carry

    lax.fori_loop(0, rows // 8, image_step, 0)

    def rms(ref):
        x = ref[...].astype(jnp.float32)
        return jnp.sqrt(jnp.sum(x * x, axis=1, keepdims=True) * (1.0 / cols) + 1e-06)

    own_scale = rms(own_ref)
    mate_scale = jnp.broadcast_to(rms(mate_ref), (mates, LANES)).T[:1, :]
    scores = best[...] / (math.sqrt(cols) * own_scale * mate_scale)
    best[...] = scores
    turned_ref[...] = scores.T
    share = mine_ref.shape[0]
    mine_ref[...] = best[pl.ds(pl.multiple_of(info[0] * share, share), share), :]
    other_ref[...] = best[pl.ds(pl.multiple_of((1 - info[0]) * share, share), share), :]


def per_device(tables, coeffs, orders, plan):
    index, there, back, sides = tables
    ang_count = lax.axis_size("ang")
    ang_index = lax.axis_index("ang")
    blk_index = lax.axis_index("blk")
    rows, cols = coeffs.shape
    share = rows // ang_count
    half = cols // 2
    route = jnp.asarray(index)[plan[0], plan[1]]
    side = jnp.asarray(sides)[route, blk_index]
    swapped = (plan[0] > plan[1]).astype(jnp.int32)
    active = (1 - side) ^ swapped
    starts = jnp.sum(orders[None, :] < jnp.arange(ORDERS + 1)[:, None], axis=1).astype(jnp.int32)
    info = jnp.concatenate([ang_index[None].astype(jnp.int32), starts])

    vmem = pl.BlockSpec(memory_space=pltpu.VMEM)
    smem = pl.BlockSpec(memory_space=pltpu.SMEM)
    params = pltpu.CompilerParams(vmem_limit_bytes=48 * 1024 * 1024)
    own, send = pl.pallas_call(
        sort_kernel,
        out_shape=(
            jax.ShapeDtypeStruct((rows, cols), jnp.bfloat16),
            jax.ShapeDtypeStruct((share, cols), jnp.bfloat16),
        ),
        in_specs=[smem, vmem, vmem],
        out_specs=(vmem, vmem),
        scratch_shapes=[pltpu.VMEM((half, half), jnp.bfloat16)],
        compiler_params=params,
    )(info, orders[None, :], coeffs)

    blk_count = lax.axis_size("blk")

    def over(value, choices, side_of_low):
        if len(choices) <= MOST_ROUTES:
            branches = [
                functools.partial(lambda pairs, v: lax.ppermute(v, "blk", pairs), pairs) for pairs in choices
            ]
            return lax.switch(route, branches, value)
        got = []
        for offset in (jnp.minimum(plan[0], plan[1]), jnp.maximum(plan[0], plan[1])):
            held = value
            for bit in range(blk_count.bit_length() - 1):
                pairs = [(b, b ^ (1 << bit)) for b in range(blk_count)]
                wanted = ((offset >> bit) & 1) == 1
                held = jnp.where(wanted, lax.ppermute(held, "blk", pairs), held)
            got.append(held)
        return jnp.where(side == side_of_low, got[0], got[1])

    mate = over(send, there, 1)
    wide = -(-share // LANES) * LANES
    mate = jnp.pad(mate, ((0, wide - share), (0, 0)))
    block = jax.ShapeDtypeStruct((share, wide), jnp.float32)
    mine, other, turned = pl.pallas_call(
        pair_kernel,
        out_shape=(block, block, jax.ShapeDtypeStruct((wide, rows), jnp.float32)),
        in_specs=[smem, vmem, vmem, vmem],
        out_specs=(vmem, vmem, vmem),
        scratch_shapes=[
            pltpu.VMEM((rows * PITCH, wide), jnp.float32),
            pltpu.VMEM((rows, 2 * wide), jnp.float32),
            pltpu.VMEM((rows, wide), jnp.float32),
        ],
        compiler_params=params,
    )(info, own, mate, jnp.asarray(angle_table()))
    sent = over(turned[:share], back, 0)
    if ang_count == 2:
        across = lax.ppermute(other, "ang", [(0, 1), (1, 0)])
        here = jnp.where(
            ang_index == 0,
            jnp.concatenate([mine, across], axis=1),
            jnp.concatenate([across, mine], axis=1),
        )
    else:
        pieces = turned[:share].T.reshape(ang_count, share, share)
        pieces = lax.all_to_all(pieces, "ang", 0, 0)
        here = pieces.transpose(1, 0, 2).reshape(share, rows)
    return jnp.where(
        active == 0, jnp.stack([here, sent]), jnp.stack([sent, here])
    )


def solution(mesh):
    in_specs = (P("blk", None), P(), P())
    out_specs = P(None, ("blk", "ang"), None)
    return jax.shard_map(
        functools.partial(per_device, routes(mesh.shape["blk"])),
        mesh=mesh,
        in_specs=in_specs,
        out_specs=out_specs,
        check_vma=False,
    )
```

```python
import functools
import math

import jax
import jax.numpy as jnp
import numpy as np
from jax import lax
from jax.experimental import pallas as pl
from jax.experimental.pallas import tpu as pltpu
from jax.sharding import PartitionSpec as P

ANGLES = 128
ORDERS = 48
ROUNDS = 2
LANES = 128
PITCH = 104
ORDER_STEP = 4
IMAGE_STEP = 16
MOST_ROUTES = 128
NT = (((1,), (1,)), ((), ()))


def low_bit(value):
    return value & -value


def side_mask(p, q):
    both = p & q
    plain = jnp.where(both != 0, low_bit(both), low_bit(p) | low_bit(q))
    odd, even = jnp.where(p & 1, p, q), jnp.where(p & 1, q, p)
    rest = even & ~odd
    mixed = jnp.where(rest != 0, 1 | low_bit(rest), plain)
    return jnp.where(both & 1, 1, jnp.where((p | q) & 1, mixed, plain | 1))


def parity(value, bits):
    return sum((value >> bit) & 1 for bit in range(bits)) & 1


def side_mask_of(p, q):
    low = lambda v: v & -v
    both = p & q
    plain = low(both) if both else low(p) | low(q)
    if both & 1:
        return 1
    if (p | q) & 1:
        odd, even = (p, q) if p & 1 else (q, p)
        rest = even & ~odd
        return 1 | low(rest) if rest else plain
    return plain | 1


def routes(n_blk):
    there, back = [], []
    for p in range(1, n_blk):
        for q in range(p, n_blk):
            mask = side_mask_of(p, q)
            assert bin(mask & p).count("1") % 2 and bin(mask & q).count("1") % 2
            pairs = [(b, b ^ (q if bin(mask & b).count("1") % 2 else p)) for b in range(n_blk)]
            assert sorted(t for _, t in pairs) == list(range(n_blk))
            there.append(pairs)
            back.append([(t, s) for s, t in pairs])
    return there, back


def angle_table():
    theta = 2.0 * math.pi * np.arange(ANGLES) / ANGLES
    phase = theta[:, None] * np.arange(ORDERS)[None, :]
    full = np.concatenate([np.cos(phase), np.sin(phase)], axis=1)
    high = full.astype(np.float32).astype(jnp.bfloat16)
    low = (full - high.astype(np.float64)).astype(np.float32).astype(jnp.bfloat16)
    return np.concatenate([high, low], axis=1)


def sort_kernel(orders_ref, x_ref, own_ref, send_ref, perm):
    half = orders_ref.shape[1]
    rows = x_ref.shape[0]
    chunks = half // LANES
    slot = lax.broadcasted_iota(jnp.int32, (1, half), 1)
    key = (orders_ref[...] * half + slot).astype(jnp.float32)
    lane = lax.broadcasted_iota(jnp.int32, (LANES, half), 1).astype(jnp.float32)
    for c in range(chunks):
        piece = key[:, c * LANES : (c + 1) * LANES]
        column = jnp.broadcast_to(piece, (LANES, LANES)).T
        count = jnp.zeros((LANES, LANES), jnp.float32)
        for d in range(chunks):
            other = key[:, d * LANES : (d + 1) * LANES]
            count += jnp.where(other < column, 1.0, 0.0)
        rank = jnp.sum(count, axis=1, keepdims=True)
        perm[c * LANES : (c + 1) * LANES, :] = jnp.where(lane == rank, 1.0, 0.0).astype(jnp.bfloat16)
    width = 2 * LANES
    for d in range(half // width):
        p = perm[:, d * width : (d + 1) * width]
        for part in range(2):
            got = jnp.dot(
                x_ref[:, part * half : (part + 1) * half], p, preferred_element_type=jnp.float32
            ).astype(jnp.bfloat16)
            for e in range(2):
                at = ((2 * d + e) * 2 + part) * LANES
                own_ref[:, at : at + LANES] = got[:, e * LANES : (e + 1) * LANES]
    share = send_ref.shape[1]
    first = pl.multiple_of(lax.axis_index("ang") * share, share)
    for at in range(0, 2 * half, LANES):
        send_ref[at : at + LANES, :] = own_ref[pl.ds(first, share), at : at + LANES].T


def pair_kernel(starts, own_ref, mate_ref, table_ref, mine_ref, other_ref, turned_ref, grid, acc, best):
    rows, cols = own_ref.shape
    mates = mate_ref.shape[1]
    width = 2 * LANES
    slots = lax.broadcasted_iota(jnp.int32, (LANES, mates), 0)

    def product(chunk, low, high):
        at = pl.multiple_of(chunk * width, width)
        place = slots + chunk * LANES
        keep = jnp.where((place >= low) & (place < high), 1.0, 0.0).astype(jnp.bfloat16)
        u = mate_ref[pl.ds(at, LANES), :] * keep
        v = mate_ref[pl.ds(at + LANES, LANES), :] * keep
        w = jnp.concatenate(
            [jnp.concatenate([u, v], axis=1), jnp.concatenate([v, -u], axis=1)], axis=0
        )
        return jnp.dot(own_ref[:, pl.ds(at, width)], w, preferred_element_type=jnp.float32)

    def spread(k, value):
        for i in range(0, rows, 8):
            grid[pl.ds(i * PITCH + k, 8, stride=PITCH), :] = value[i : i + 8, :mates]
            grid[pl.ds(i * PITCH + k + ORDERS, 8, stride=PITCH), :] = value[i : i + 8, mates:]

    def span(k):
        low, high = starts[k], starts[k + 1]
        chunk = jnp.minimum(low // LANES, cols // width - 1)
        return low, high, chunk, (high + LANES - 1) // LANES

    def first_chunks(step, carry):
        for k in range(ORDER_STEP):
            low, high, chunk, _ = span(step * ORDER_STEP + k)
            spread(step * ORDER_STEP + k, product(chunk, low, high))
        return carry

    lax.fori_loop(0, ORDERS // ORDER_STEP, first_chunks, 0)

    def wide_orders(k, carry):
        low, high, chunk, last = span(k)

        @pl.when(last > chunk + 1)
        def _():
            acc[...] = jnp.zeros_like(acc)

            def more(c, carry):
                acc[...] += product(c, low, high)
                return carry

            lax.fori_loop(chunk, last, more, 0)
            spread(k, acc[...])

        return carry

    lax.fori_loop(0, ORDERS, wide_orders, 0)

    table = table_ref[...]

    def image_step(step, carry):
        base = pl.multiple_of(step * IMAGE_STEP, IMAGE_STEP)
        rows_out = []
        for i in range(0, IMAGE_STEP, 2):
            pieces = []
            for e in range(2):
                at = pl.multiple_of((base + i + e) * PITCH, 8)
                pieces.append(grid[pl.ds(at, 2 * ORDERS), :].astype(jnp.bfloat16))
            d = jnp.concatenate(pieces, axis=1)
            d = jnp.concatenate([d, d], axis=0)
            raw = jnp.dot(table, d, preferred_element_type=jnp.float32)
            top = jnp.max(raw, axis=0, keepdims=True)
            rows_out += [top[:, :mates], top[:, mates:]]
        best[pl.ds(base, IMAGE_STEP), :] = jnp.concatenate(rows_out, axis=0)
        return carry

    lax.fori_loop(0, rows // IMAGE_STEP, image_step, 0)

    def rms(ref, axis):
        x = ref[...].astype(jnp.float32)
        return jnp.sqrt(jnp.sum(x * x, axis=axis, keepdims=True) * (1.0 / cols) + 1e-06)

    scores = best[...] / (math.sqrt(cols) * rms(own_ref, 1) * rms(mate_ref, 0))
    best[...] = scores
    turned_ref[...] = scores.T
    share = mine_ref.shape[0]
    ang = lax.axis_index("ang")
    mine_ref[...] = best[pl.ds(pl.multiple_of(ang * share, share), share), :]
    if other_ref.shape[0] * 2 == rows:
        other_ref[...] = best[pl.ds(pl.multiple_of((1 - ang) * share, share), share), :]
    else:
        other_ref[...] = jnp.zeros_like(other_ref)


def per_device(tables, coeffs, orders, plan):
    there, back = tables
    ang_count = lax.axis_size("ang")
    ang_index = lax.axis_index("ang")
    blk_index = lax.axis_index("blk")
    rows, cols = coeffs.shape
    share = rows // ang_count
    half = cols // 2
    blk_count = lax.axis_size("blk")
    low, high = jnp.minimum(plan[0], plan[1]), jnp.maximum(plan[0], plan[1])
    route = (low - 1) * blk_count - (low - 1) * low // 2 + high - low
    side = parity(side_mask(low, high) & blk_index, blk_count.bit_length() - 1)
    swapped = (plan[0] > plan[1]).astype(jnp.int32)
    active = (1 - side) ^ swapped
    starts = jnp.sum(orders[None, :] < jnp.arange(ORDERS + 1)[:, None], axis=1).astype(jnp.int32)

    vmem = pl.BlockSpec(memory_space=pltpu.VMEM)
    smem = pl.BlockSpec(memory_space=pltpu.SMEM)
    params = pltpu.CompilerParams(vmem_limit_bytes=48 * 1024 * 1024)
    own, send = pl.pallas_call(
        sort_kernel,
        out_shape=(
            jax.ShapeDtypeStruct((rows, cols), jnp.bfloat16),
            jax.ShapeDtypeStruct((cols, share), jnp.bfloat16),
        ),
        in_specs=[vmem, vmem],
        out_specs=(vmem, vmem),
        scratch_shapes=[pltpu.VMEM((half, half), jnp.bfloat16)],
        compiler_params=params,
    )(orders[None, :], coeffs)

    def over(value, choices, side_of_low):
        if len(choices) <= MOST_ROUTES:
            branches = [
                functools.partial(lambda pairs, v: lax.ppermute(v, "blk", pairs), pairs) for pairs in choices
            ]
            return lax.switch(route, branches, value)
        got = []
        for offset in (low, high):
            held = value
            for bit in range(blk_count.bit_length() - 1):
                pairs = [(b, b ^ (1 << bit)) for b in range(blk_count)]
                wanted = ((offset >> bit) & 1) == 1
                held = jnp.where(wanted, lax.ppermute(held, "blk", pairs), held)
            got.append(held)
        return jnp.where(side == side_of_low, got[0], got[1])

    mate = over(send, there, 1)
    wide = -(-share // LANES) * LANES
    mate = jnp.pad(mate, ((0, 0), (0, wide - share)))
    block = jax.ShapeDtypeStruct((share, wide), jnp.float32)
    mine, other, turned = pl.pallas_call(
        pair_kernel,
        out_shape=(block, block, jax.ShapeDtypeStruct((wide, rows), jnp.float32)),
        in_specs=[smem, vmem, vmem, vmem],
        out_specs=(vmem, vmem, vmem),
        scratch_shapes=[
            pltpu.VMEM((rows * PITCH, wide), jnp.float32),
            pltpu.VMEM((rows, 2 * wide), jnp.float32),
            pltpu.VMEM((rows, wide), jnp.float32),
        ],
        compiler_params=params,
    )(starts, own, mate, jnp.asarray(angle_table()))
    sent = over(turned[:share], back, 0)
    if ang_count == 2:
        across = lax.ppermute(other, "ang", [(0, 1), (1, 0)])
        here = jnp.where(
            ang_index == 0,
            jnp.concatenate([mine, across], axis=1),
            jnp.concatenate([across, mine], axis=1),
        )
    else:
        pieces = turned[:share].T.reshape(ang_count, share, share)
        pieces = lax.all_to_all(pieces, "ang", 0, 0)
        here = pieces.transpose(1, 0, 2).reshape(share, rows)
    return jnp.where(
        active == 0, jnp.stack([here, sent]), jnp.stack([sent, here])
    )


def solution(mesh):
    in_specs = (P("blk", None), P(), P())
    out_specs = P(None, ("blk", "ang"), None)
    return jax.shard_map(
        functools.partial(per_device, routes(mesh.shape["blk"])),
        mesh=mesh,
        in_specs=in_specs,
        out_specs=out_specs,
        check_vma=False,
    )
```

```python
import functools
import math

import jax
import jax.numpy as jnp
import numpy as np
from jax import lax
from jax.experimental import pallas as pl
from jax.experimental.pallas import tpu as pltpu
from jax.sharding import PartitionSpec as P

ANGLES = 128
ORDERS = 48
ROUNDS = 2
LANES = 128
PITCH = 97
ORDER_STEP = 16
IMAGE_STEP = 64
MOST_ROUTES = 128
NT = (((1,), (1,)), ((), ()))


def low_bit(value):
    return value & -value


def side_mask(p, q):
    both = p & q
    plain = jnp.where(both != 0, low_bit(both), low_bit(p) | low_bit(q))
    odd, even = jnp.where(p & 1, p, q), jnp.where(p & 1, q, p)
    rest = even & ~odd
    mixed = jnp.where(rest != 0, 1 | low_bit(rest), plain)
    return jnp.where(both & 1, 1, jnp.where((p | q) & 1, mixed, plain | 1))


def parity(value, bits):
    return sum((value >> bit) & 1 for bit in range(bits)) & 1


def side_mask_of(p, q):
    low = lambda v: v & -v
    both = p & q
    plain = low(both) if both else low(p) | low(q)
    if both & 1:
        return 1
    if (p | q) & 1:
        odd, even = (p, q) if p & 1 else (q, p)
        rest = even & ~odd
        return 1 | low(rest) if rest else plain
    return plain | 1


def routes(n_blk):
    there, back = [], []
    for p in range(1, n_blk):
        for q in range(p, n_blk):
            mask = side_mask_of(p, q)
            assert bin(mask & p).count("1") % 2 and bin(mask & q).count("1") % 2
            pairs = [(b, b ^ (q if bin(mask & b).count("1") % 2 else p)) for b in range(n_blk)]
            assert sorted(t for _, t in pairs) == list(range(n_blk))
            there.append(pairs)
            back.append([(t, s) for s, t in pairs])
    return there, back


def angle_table():
    theta = 2.0 * math.pi * np.arange(ANGLES) / ANGLES
    phase = theta[:, None] * np.arange(ORDERS)[None, :]
    full = np.concatenate([np.cos(phase), np.sin(phase)], axis=1)
    high = full.astype(np.float32).astype(jnp.bfloat16)
    low = (full - high.astype(np.float64)).astype(np.float32).astype(jnp.bfloat16)
    return np.concatenate([high, low], axis=1)


def sort_kernel(orders_ref, x_hbm, own_ref, send_ref, perm, x_ref, arrived):
    fetch = pltpu.make_async_copy(x_hbm, x_ref, arrived)
    fetch.start()
    half = orders_ref.shape[1]
    chunks = half // LANES
    slot = lax.broadcasted_iota(jnp.int32, (1, half), 1)
    key = (orders_ref[...] * half + slot).astype(jnp.float32)
    lane = lax.broadcasted_iota(jnp.int32, (LANES, half), 1).astype(jnp.float32)
    for c in range(chunks):
        piece = key[:, c * LANES : (c + 1) * LANES]
        column = jnp.broadcast_to(piece, (LANES, LANES)).T
        count = jnp.zeros((LANES, LANES), jnp.float32)
        for d in range(chunks):
            other = key[:, d * LANES : (d + 1) * LANES]
            count += jnp.where(other < column, 1.0, 0.0)
        rank = jnp.sum(count, axis=1, keepdims=True)
        perm[c * LANES : (c + 1) * LANES, :] = jnp.where(lane == rank, 1.0, 0.0).astype(jnp.bfloat16)
    fetch.wait()
    width = 2 * LANES
    for d in range(half // width):
        p = perm[:, d * width : (d + 1) * width]
        for part in range(2):
            got = jnp.dot(
                x_ref[:, part * half : (part + 1) * half], p, preferred_element_type=jnp.float32
            ).astype(jnp.bfloat16)
            for e in range(2):
                at = ((2 * d + e) * 2 + part) * LANES
                own_ref[:, at : at + LANES] = got[:, e * LANES : (e + 1) * LANES]
    share = send_ref.shape[1]
    first = pl.multiple_of(lax.axis_index("ang") * share, share)
    for at in range(0, 2 * half, LANES):
        send_ref[at : at + LANES, :] = own_ref[pl.ds(first, share), at : at + LANES].T


def pair_kernel(starts, heads, own_ref, mate_ref, table_ref, mine_ref, other_ref, turned_ref, grid, best):
    rows, cols = own_ref.shape
    mates = mate_ref.shape[1]
    width = 2 * LANES
    slots = lax.broadcasted_iota(jnp.int32, (LANES, mates), 0)

    def product(chunk, low, high):
        at = chunk * width if isinstance(chunk, int) else pl.multiple_of(chunk * width, width)
        place = slots + chunk * LANES
        keep = jnp.where((place >= low) & (place < high), 1.0, 0.0).astype(jnp.bfloat16)
        u = mate_ref[pl.ds(at, LANES), :] * keep
        v = mate_ref[pl.ds(at + LANES, LANES), :] * keep
        w = jnp.concatenate(
            [jnp.concatenate([u, v], axis=1), jnp.concatenate([v, -u], axis=1)], axis=0
        )
        return jnp.dot(own_ref[:, pl.ds(at, width)], w, preferred_element_type=jnp.float32)

    def spread(k, value):
        for i in range(0, rows, 8):
            grid[pl.ds(i * PITCH + k, 8, stride=PITCH), :] = value[i : i + 8, :mates]
            grid[pl.ds(i * PITCH + k + ORDERS, 8, stride=PITCH), :] = value[i : i + 8, mates:]

    def first_chunks(step, carry):
        for e in range(ORDER_STEP):
            k = step * ORDER_STEP + e
            low = starts[k]
            spread(k, product(jnp.minimum(low // LANES, cols // width - 1), low, starts[k + 1]))
        return carry

    lax.fori_loop(0, ORDERS // ORDER_STEP, first_chunks, 0)

    for chunk in range(1, cols // width):
        k = heads[chunk]
        low = jnp.where(starts[k] < chunk * LANES, starts[k], starts[k + 1])
        value = product(chunk, low, starts[k + 1])
        for i in range(0, rows, 8):
            cos_at = pl.ds(i * PITCH + k, 8, stride=PITCH)
            sin_at = pl.ds(i * PITCH + k + ORDERS, 8, stride=PITCH)
            grid[cos_at, :] += value[i : i + 8, :mates]
            grid[sin_at, :] += value[i : i + 8, mates:]

    table = table_ref[...]

    def image_step(step, carry):
        base = pl.multiple_of(step * IMAGE_STEP, IMAGE_STEP)
        rows_out = []
        for i in range(0, IMAGE_STEP, 2):
            pieces = []
            for e in range(2):
                at = (base + i + e) * PITCH
                pieces.append(grid[pl.ds(at, 2 * ORDERS), :].astype(jnp.bfloat16))
            d = jnp.concatenate(pieces, axis=1)
            d = jnp.concatenate([d, d], axis=0)
            raw = jnp.dot(table, d, preferred_element_type=jnp.float32)
            top = jnp.max(raw, axis=0, keepdims=True)
            rows_out += [top[:, :mates], top[:, mates:]]
        best[pl.ds(base, IMAGE_STEP), :] = jnp.concatenate(rows_out, axis=0)
        return carry

    lax.fori_loop(0, rows // IMAGE_STEP, image_step, 0)

    def rms(ref, axis):
        x = ref[...].astype(jnp.float32)
        return jnp.sqrt(jnp.sum(x * x, axis=axis, keepdims=True) * (1.0 / cols) + 1e-06)

    scores = best[...] / (math.sqrt(cols) * rms(own_ref, 1) * rms(mate_ref, 0))
    best[...] = scores
    turned_ref[...] = scores.T
    share = mine_ref.shape[0]
    ang = lax.axis_index("ang")
    mine_ref[...] = best[pl.ds(pl.multiple_of(ang * share, share), share), :]
    if other_ref.shape[0] * 2 == rows:
        other_ref[...] = best[pl.ds(pl.multiple_of((1 - ang) * share, share), share), :]
    else:
        other_ref[...] = jnp.zeros_like(other_ref)


def per_device(tables, coeffs, orders, plan):
    there, back = tables
    ang_count = lax.axis_size("ang")
    ang_index = lax.axis_index("ang")
    blk_index = lax.axis_index("blk")
    rows, cols = coeffs.shape
    share = rows // ang_count
    half = cols // 2
    blk_count = lax.axis_size("blk")
    low, high = jnp.minimum(plan[0], plan[1]), jnp.maximum(plan[0], plan[1])
    route = (low - 1) * blk_count - (((low - 1) * low) >> 1) + high - low
    side = parity(side_mask(low, high) & blk_index, blk_count.bit_length() - 1)
    swapped = (plan[0] > plan[1]).astype(jnp.int32)
    active = (1 - side) ^ swapped
    starts = jnp.sum(orders[None, :] < jnp.arange(ORDERS + 1)[:, None], axis=1).astype(jnp.int32)
    firsts = jnp.arange(half // LANES) * LANES
    heads = jnp.sum(starts[1:, None] <= firsts[None, :], axis=0).astype(jnp.int32)

    vmem = pl.BlockSpec(memory_space=pltpu.VMEM)
    smem = pl.BlockSpec(memory_space=pltpu.SMEM)
    params = pltpu.CompilerParams(vmem_limit_bytes=48 * 1024 * 1024)
    own, send = pl.pallas_call(
        sort_kernel,
        out_shape=(
            jax.ShapeDtypeStruct((rows, cols), jnp.bfloat16),
            jax.ShapeDtypeStruct((cols, share), jnp.bfloat16),
        ),
        in_specs=[vmem, pl.BlockSpec(memory_space=pltpu.HBM)],
        out_specs=(vmem, vmem),
        scratch_shapes=[
            pltpu.VMEM((half, half), jnp.bfloat16),
            pltpu.VMEM((rows, cols), jnp.bfloat16),
            pltpu.SemaphoreType.DMA,
        ],
        compiler_params=params,
    )(orders[None, :], coeffs)

    def over(value, choices, side_of_low):
        if len(choices) <= MOST_ROUTES:
            branches = [
                functools.partial(lambda pairs, v: lax.ppermute(v, "blk", pairs), pairs) for pairs in choices
            ]
            return lax.switch(route, branches, value)
        got = []
        for offset in (low, high):
            held = value
            for bit in range(blk_count.bit_length() - 1):
                pairs = [(b, b ^ (1 << bit)) for b in range(blk_count)]
                wanted = ((offset >> bit) & 1) == 1
                held = jnp.where(wanted, lax.ppermute(held, "blk", pairs), held)
            got.append(held)
        return jnp.where(side == side_of_low, got[0], got[1])

    mate = over(send, there, 1)
    wide = -(-share // LANES) * LANES
    mate = jnp.pad(mate, ((0, 0), (0, wide - share)))
    block = jax.ShapeDtypeStruct((share, wide), jnp.float32)
    mine, other, turned = pl.pallas_call(
        pair_kernel,
        out_shape=(block, block, jax.ShapeDtypeStruct((wide, rows), jnp.float32)),
        in_specs=[smem, smem, vmem, vmem, vmem],
        out_specs=(vmem, vmem, vmem),
        scratch_shapes=[
            pltpu.VMEM((rows * PITCH, wide), jnp.float32),
            pltpu.VMEM((rows, wide), jnp.float32),
        ],
        compiler_params=params,
    )(starts, heads, own, mate, jnp.asarray(angle_table()))
    sent = over(turned[:share], back, 0)
    if ang_count == 2:
        across = lax.ppermute(other, "ang", [(0, 1), (1, 0)])
        here = jnp.where(
            ang_index == 0,
            jnp.concatenate([mine, across], axis=1),
            jnp.concatenate([across, mine], axis=1),
        )
    else:
        pieces = turned[:share].T.reshape(ang_count, share, share)
        pieces = lax.all_to_all(pieces, "ang", 0, 0)
        here = pieces.transpose(1, 0, 2).reshape(share, rows)
    return jnp.where(
        active == 0, jnp.stack([here, sent]), jnp.stack([sent, here])
    )


def solution(mesh):
    in_specs = (P("blk", None), P(), P())
    out_specs = P(None, ("blk", "ang"), None)
    return jax.shard_map(
        functools.partial(per_device, routes(mesh.shape["blk"])),
        mesh=mesh,
        in_specs=in_specs,
        out_specs=out_specs,
        check_vma=False,
    )
```

```python
import functools
import math

import jax
import jax.numpy as jnp
import numpy as np
from jax import lax
from jax.experimental import pallas as pl
from jax.experimental.pallas import tpu as pltpu
from jax.sharding import PartitionSpec as P

ANGLES = 128
ORDERS = 48
ROUNDS = 2
LANES = 128
PITCH = 97
ORDER_STEP = 16
IMAGE_STEP = 64
MOST_ROUTES = 128
NT = (((1,), (1,)), ((), ()))


def low_bit(value):
    return value & -value


def side_mask(p, q):
    both = p & q
    plain = jnp.where(both != 0, low_bit(both), low_bit(p) | low_bit(q))
    odd, even = jnp.where(p & 1, p, q), jnp.where(p & 1, q, p)
    rest = even & ~odd
    mixed = jnp.where(rest != 0, 1 | low_bit(rest), plain)
    return jnp.where(both & 1, 1, jnp.where((p | q) & 1, mixed, plain | 1))


def parity(value, bits):
    return sum((value >> bit) & 1 for bit in range(bits)) & 1


def side_mask_of(p, q):
    low = lambda v: v & -v
    both = p & q
    plain = low(both) if both else low(p) | low(q)
    if both & 1:
        return 1
    if (p | q) & 1:
        odd, even = (p, q) if p & 1 else (q, p)
        rest = even & ~odd
        return 1 | low(rest) if rest else plain
    return plain | 1


def routes(n_blk):
    there, back = [], []
    for p in range(1, n_blk):
        for q in range(p, n_blk):
            mask = side_mask_of(p, q)
            assert bin(mask & p).count("1") % 2 and bin(mask & q).count("1") % 2
            pairs = [(b, b ^ (q if bin(mask & b).count("1") % 2 else p)) for b in range(n_blk)]
            assert sorted(t for _, t in pairs) == list(range(n_blk))
            there.append(pairs)
            back.append([(t, s) for s, t in pairs])
    return there, back


def angle_table():
    theta = 2.0 * math.pi * np.arange(ANGLES) / ANGLES
    phase = theta[:, None] * np.arange(ORDERS)[None, :]
    full = np.concatenate([np.cos(phase), np.sin(phase)], axis=1)
    high = full.astype(np.float32).astype(jnp.bfloat16)
    low = (full - high.astype(np.float64)).astype(np.float32).astype(jnp.bfloat16)
    return np.concatenate([high, low], axis=1)


def sort_kernel(plan_ref, orders_ref, x_hbm, own_ref, send_ref, route_ref, perm, x_ref, arrived):
    fetch = pltpu.make_async_copy(x_hbm, x_ref, arrived)
    fetch.start()
    blk_count = lax.axis_size("blk")
    low, high = jnp.minimum(plan_ref[0], plan_ref[1]), jnp.maximum(plan_ref[0], plan_ref[1])
    side = parity(side_mask(low, high) & lax.axis_index("blk"), blk_count.bit_length() - 1)
    route_ref[0] = (low - 1) * blk_count - (((low - 1) * low) >> 1) + high - low
    route_ref[1] = side
    route_ref[2] = (1 - side) ^ jnp.where(plan_ref[0] > plan_ref[1], 1, 0)
    half = orders_ref.shape[1]
    chunks = half // LANES
    slot = lax.broadcasted_iota(jnp.int32, (1, half), 1)
    key = (orders_ref[...] * half + slot).astype(jnp.float32)
    lane = lax.broadcasted_iota(jnp.int32, (LANES, half), 1).astype(jnp.float32)
    for c in range(chunks):
        piece = key[:, c * LANES : (c + 1) * LANES]
        column = jnp.broadcast_to(piece, (LANES, LANES)).T
        count = jnp.zeros((LANES, LANES), jnp.float32)
        for d in range(chunks):
            other = key[:, d * LANES : (d + 1) * LANES]
            count += jnp.where(other < column, 1.0, 0.0)
        rank = jnp.sum(count, axis=1, keepdims=True)
        perm[c * LANES : (c + 1) * LANES, :] = jnp.where(lane == rank, 1.0, 0.0).astype(jnp.bfloat16)
    fetch.wait()
    width = 2 * LANES
    for d in range(half // width):
        p = perm[:, d * width : (d + 1) * width]
        for part in range(2):
            got = jnp.dot(
                x_ref[:, part * half : (part + 1) * half], p, preferred_element_type=jnp.float32
            ).astype(jnp.bfloat16)
            for e in range(2):
                at = ((2 * d + e) * 2 + part) * LANES
                own_ref[:, at : at + LANES] = got[:, e * LANES : (e + 1) * LANES]
    share = send_ref.shape[1]
    first = pl.multiple_of(lax.axis_index("ang") * share, share)
    for at in range(0, 2 * half, LANES):
        send_ref[at : at + LANES, :] = own_ref[pl.ds(first, share), at : at + LANES].T


def pair_kernel(starts, heads, own_ref, mate_ref, table_ref, mine_ref, other_ref, turned_ref, grid, best):
    rows, cols = own_ref.shape
    mates = mate_ref.shape[1]
    width = 2 * LANES
    slots = lax.broadcasted_iota(jnp.int32, (LANES, mates), 0)

    def product(chunk, low, high):
        at = chunk * width if isinstance(chunk, int) else pl.multiple_of(chunk * width, width)
        place = slots + chunk * LANES
        keep = jnp.where((place >= low) & (place < high), 1.0, 0.0).astype(jnp.bfloat16)
        u = mate_ref[pl.ds(at, LANES), :] * keep
        v = mate_ref[pl.ds(at + LANES, LANES), :] * keep
        w = jnp.concatenate(
            [jnp.concatenate([u, v], axis=1), jnp.concatenate([v, -u], axis=1)], axis=0
        )
        return jnp.dot(own_ref[:, pl.ds(at, width)], w, preferred_element_type=jnp.float32)

    def spread(k, value):
        for i in range(0, rows, 8):
            grid[pl.ds(i * PITCH + k, 8, stride=PITCH), :] = value[i : i + 8, :mates]
            grid[pl.ds(i * PITCH + k + ORDERS, 8, stride=PITCH), :] = value[i : i + 8, mates:]

    def first_chunks(step, carry):
        for e in range(ORDER_STEP):
            k = step * ORDER_STEP + e
            low = starts[k]
            spread(k, product(jnp.minimum(low // LANES, cols // width - 1), low, starts[k + 1]))
        return carry

    lax.fori_loop(0, ORDERS // ORDER_STEP, first_chunks, 0)

    for chunk in range(1, cols // width):
        k = heads[chunk]
        low = jnp.where(starts[k] < chunk * LANES, starts[k], starts[k + 1])
        value = product(chunk, low, starts[k + 1])
        for i in range(0, rows, 8):
            cos_at = pl.ds(i * PITCH + k, 8, stride=PITCH)
            sin_at = pl.ds(i * PITCH + k + ORDERS, 8, stride=PITCH)
            grid[cos_at, :] += value[i : i + 8, :mates]
            grid[sin_at, :] += value[i : i + 8, mates:]

    table = table_ref[...]

    def image_step(step, carry):
        base = pl.multiple_of(step * IMAGE_STEP, IMAGE_STEP)
        rows_out = []
        for i in range(0, IMAGE_STEP, 2):
            pieces = []
            for e in range(2):
                at = (base + i + e) * PITCH
                pieces.append(grid[pl.ds(at, 2 * ORDERS), :].astype(jnp.bfloat16))
            d = jnp.concatenate(pieces, axis=1)
            d = jnp.concatenate([d, d], axis=0)
            raw = jnp.dot(table, d, preferred_element_type=jnp.float32)
            top = jnp.max(raw, axis=0, keepdims=True)
            rows_out += [top[:, :mates], top[:, mates:]]
        best[pl.ds(base, IMAGE_STEP), :] = jnp.concatenate(rows_out, axis=0)
        return carry

    lax.fori_loop(0, rows // IMAGE_STEP, image_step, 0)

    def rms(ref, axis):
        x = ref[...].astype(jnp.float32)
        return jnp.sqrt(jnp.sum(x * x, axis=axis, keepdims=True) * (1.0 / cols) + 1e-06)

    scores = best[...] / (math.sqrt(cols) * rms(own_ref, 1) * rms(mate_ref, 0))
    best[...] = scores
    turned_ref[...] = scores.T
    share = mine_ref.shape[0]
    ang = lax.axis_index("ang")
    mine_ref[...] = best[pl.ds(pl.multiple_of(ang * share, share), share), :]
    if other_ref.shape[0] * 2 == rows:
        other_ref[...] = best[pl.ds(pl.multiple_of((1 - ang) * share, share), share), :]
    else:
        other_ref[...] = jnp.zeros_like(other_ref)


def per_device(tables, coeffs, orders, plan):
    there, back = tables
    ang_count = lax.axis_size("ang")
    ang_index = lax.axis_index("ang")
    rows, cols = coeffs.shape
    share = rows // ang_count
    half = cols // 2
    blk_count = lax.axis_size("blk")
    low, high = jnp.minimum(plan[0], plan[1]), jnp.maximum(plan[0], plan[1])
    starts = jnp.sum(orders[None, :] < jnp.arange(ORDERS + 1)[:, None], axis=1).astype(jnp.int32)
    firsts = jnp.arange(half // LANES) * LANES
    heads = jnp.sum(starts[1:, None] <= firsts[None, :], axis=0).astype(jnp.int32)

    vmem = pl.BlockSpec(memory_space=pltpu.VMEM)
    smem = pl.BlockSpec(memory_space=pltpu.SMEM)
    params = pltpu.CompilerParams(vmem_limit_bytes=48 * 1024 * 1024)
    own, send, chosen = pl.pallas_call(
        sort_kernel,
        out_shape=(
            jax.ShapeDtypeStruct((rows, cols), jnp.bfloat16),
            jax.ShapeDtypeStruct((cols, share), jnp.bfloat16),
            jax.ShapeDtypeStruct((3,), jnp.int32),
        ),
        in_specs=[smem, vmem, pl.BlockSpec(memory_space=pltpu.HBM)],
        out_specs=(vmem, vmem, smem),
        scratch_shapes=[
            pltpu.VMEM((half, half), jnp.bfloat16),
            pltpu.VMEM((rows, cols), jnp.bfloat16),
            pltpu.SemaphoreType.DMA,
        ],
        compiler_params=params,
    )(plan, orders[None, :], coeffs)
    route, side, active = chosen[0], chosen[1], chosen[2]

    def over(value, choices, side_of_low):
        if len(choices) <= MOST_ROUTES:
            branches = [
                functools.partial(lambda pairs, v: lax.ppermute(v, "blk", pairs), pairs) for pairs in choices
            ]
            return lax.switch(route, branches, value)
        got = []
        for offset in (low, high):
            held = value
            for bit in range(blk_count.bit_length() - 1):
                pairs = [(b, b ^ (1 << bit)) for b in range(blk_count)]
                wanted = ((offset >> bit) & 1) == 1
                held = jnp.where(wanted, lax.ppermute(held, "blk", pairs), held)
            got.append(held)
        return jnp.where(side == side_of_low, got[0], got[1])

    mate = over(send, there, 1)
    wide = -(-share // LANES) * LANES
    mate = jnp.pad(mate, ((0, 0), (0, wide - share)))
    block = jax.ShapeDtypeStruct((share, wide), jnp.float32)
    mine, other, turned = pl.pallas_call(
        pair_kernel,
        out_shape=(block, block, jax.ShapeDtypeStruct((wide, rows), jnp.float32)),
        in_specs=[smem, smem, vmem, vmem, vmem],
        out_specs=(vmem, vmem, vmem),
        scratch_shapes=[
            pltpu.VMEM((rows * PITCH, wide), jnp.float32),
            pltpu.VMEM((rows, wide), jnp.float32),
        ],
        compiler_params=params,
    )(starts, heads, own, mate, jnp.asarray(angle_table()))
    sent = over(turned[:share], back, 0)
    if ang_count == 2:
        across = lax.ppermute(other, "ang", [(0, 1), (1, 0)])
        here = jnp.where(
            ang_index == 0,
            jnp.concatenate([mine, across], axis=1),
            jnp.concatenate([across, mine], axis=1),
        )
    else:
        pieces = turned[:share].T.reshape(ang_count, share, share)
        pieces = lax.all_to_all(pieces, "ang", 0, 0)
        here = pieces.transpose(1, 0, 2).reshape(share, rows)
    return jnp.where(
        active == 0, jnp.stack([here, sent]), jnp.stack([sent, here])
    )


def solution(mesh):
    in_specs = (P("blk", None), P(), P())
    out_specs = P(None, ("blk", "ang"), None)
    return jax.shard_map(
        functools.partial(per_device, routes(mesh.shape["blk"])),
        mesh=mesh,
        in_specs=in_specs,
        out_specs=out_specs,
        check_vma=False,
    )
```
